32 devices in a mesh: row: 4 (over z), col: 8 (over y, x, core).
Axes of the slice: x: 2, y: 2, z: 4, core: 2. Of those that a mesh axis runs over, the one named last changes fastest.
Arguments:
- matrix: float32 [32, 512, 16, 1024], P(None, 'row', None, 'col'), may hold values from -150 to 150
- inverse_rest: float32 [32, 512, 14, 1024], P(None, 'row', None, 'col'), may hold values from -6 to 6
- upper_block: float32 [4, 512, 2, 1024], P(None, 'row', None, 'col'), may hold values from -6 to 6, as said below
- lower_below: float32 [4, 512, 14, 1024], P(None, 'row', None, 'col'), may hold values from -0.046875 to 0.046875
- lower_inverse: float32 [4, 512, 2048], P(None, 'row', 'col'), may hold values from -1 to 1, as said below
Outputs:
- plus_rows: float32 [4, 512, 16, 1024], P(None, 'row', None, 'col')
The draws below stay inside these ranges and needn't reach their ends.
Inputs may be any that keep to these rules, and one draw needn't show every extreme that they name: `upper_block`: upper triangular. `lower_inverse`: unit lower triangular.
All inputs are finite; a program needn't handle non-finite values.
Results may differ from the reference program's by a relative error of at most 0.000052.
Values sent between devices are 32-bit elements; how exact they have to be, the bound alone decides.
A program may use at most 256 MiB of HBM per device.

```python
import jax
import jax.numpy as jnp
from jax import lax

N = 16384
BLK = 128
W = 2048
REST = 14336
KR = 32
KC = 16
KWR = 4
KW = 2
KCR = 14
N_ROW = 4
N_COL = 8


def draw_matrix(key, part):
    row_key, col_key, base_key = jax.random.split(jax.random.fold_in(key, 17), 3)
    row_scale = jnp.exp(jax.random.uniform(row_key, (N, 1), jnp.float32, 0.0, 2.302585))
    col_scale = jnp.exp(jax.random.uniform(col_key, (1, N), jnp.float32, 0.0, 2.302585))
    values = jnp.clip(jax.random.normal(base_key, (N, N), jnp.float32), -6.0, 6.0)
    return (values * row_scale * col_scale * 0.25).reshape(KR, N // KR, KC, N // KC)


def draw_upper_block(key, part):
    base_key = jax.random.fold_in(key, 23)
    values = jnp.clip(jax.random.normal(base_key, (W, W), jnp.float32), -6.0, 6.0)
    return jnp.triu(values).reshape(KWR, W // KWR, KW, W // KW)


def draw_lower_inverse(key, part):
    base_key = jax.random.fold_in(key, 29)
    values = jnp.clip(jax.random.normal(base_key, (W, W), jnp.float32), -6.0, 6.0) * (0.5 / jnp.sqrt(W * 1.0))
    unit_lower = jnp.eye(W, dtype=jnp.float32) + jnp.tril(values, -1)
    return unit_lower.reshape(KWR, W // KWR, W)


def block_levels(own_key, extent, cuts, smallest, largest):
    loudness = 1.0
    for axis_at, blocks in cuts:
        draws = jax.random.uniform(jax.random.fold_in(jax.random.fold_in(own_key, 6), axis_at), (blocks,), jnp.float32, smallest / len(cuts), largest / len(cuts))
        loudness = loudness * jnp.repeat(jnp.exp(draws), extent[axis_at] // blocks).reshape((-1,) + (1,) * (len(extent) - 1 - axis_at))
    return loudness


def noise(key, dims, spread, reach, pieces=(), held_as=jnp.bfloat16):
    values = spread * jax.random.normal(key, dims, jnp.float32)
    if pieces:
        values = values * block_levels(key, dims, pieces, -0.22, 0.18)
    return jnp.clip(values, -reach, reach).astype(held_as)


def setup_inputs(seed: int = 0) -> dict:
    seeds = jax.random.split(jax.random.key(seed), 6)
    matrix = draw_matrix(jax.random.fold_in(seeds[5], 71), 0)
    inverse_rest = noise(seeds[1], (KR, N_ROW * BLK, KCR, N_COL * BLK), 1.0, 6.0, ((1, 4), (3, 8)), jnp.float32)
    upper_block = draw_upper_block(jax.random.fold_in(seeds[5], 71), 0)
    lower_below = noise(seeds[3], (KWR, N_ROW * BLK, KCR, N_COL * BLK), REST ** -0.5, 0.046875, ((1, 4), (3, 8)), jnp.float32)
    lower_inverse = draw_lower_inverse(jax.random.fold_in(seeds[5], 71), 0)
    return {"matrix": matrix, "inverse_rest": inverse_rest, "upper_block": upper_block, "lower_below": lower_below, "lower_inverse": lower_inverse}


def reference(matrix, inverse_rest, upper_block, lower_below, lower_inverse):
    whole_matrix = matrix.reshape(N, N)
    rest_inverse = inverse_rest.reshape(N, N - W)
    upper_part = upper_block.reshape(W, W)
    below_part = lower_below.reshape(W, N - W)
    factor_part = lower_inverse.reshape(W, W)
    correction = jnp.dot(rest_inverse, below_part.T, precision=lax.Precision.HIGHEST, preferred_element_type=jnp.float32)
    update_panel = jnp.concatenate([upper_part, jnp.zeros((N - W, W), jnp.float32)], axis=0) - correction
    inverse_panel = jnp.dot(update_panel, factor_part, precision=lax.Precision.HIGHEST, preferred_element_type=jnp.float32)
    matrix_norm = jnp.sum(whole_matrix * whole_matrix)
    inverse_norm = jnp.sum(rest_inverse * rest_inverse) + jnp.sum(inverse_panel * inverse_panel)
    balance = jnp.sqrt(jnp.sqrt(inverse_norm / matrix_norm))
    plus_rows = 0.5 * (balance * whole_matrix[:W] + inverse_panel.T / balance)
    return plus_rows.reshape(KWR, W // KWR, KC, N // KC)
```

```python
import functools

import jax
import jax.numpy as jnp
from jax import lax
from jax.experimental import pallas as pl
from jax.experimental.pallas import tpu as pltpu
from jax.sharding import PartitionSpec as P

MESH = pl.DeviceIdType.MESH


def halvings(col_devices):
    bits = col_devices.bit_length() - 1
    return [[0] + list(range(1, bits)), [0] + list(range(bits - 1, 0, -1))]


def held(order, stage, col_devices):
    cleared = sum(1 << b for b in order[: stage + 1])
    return [m for m in range(col_devices) if m & cleared == 0]


def panel_kernel(
    rows_n, cols_n, steps_of,
    matrix_ref, rest_ref, below_ref, upper_ref, lower_ref, mirror_ref, factor_ref, total_ref,
    land, raw, left, right, sums, update, pair, tile, total, outbox, squares, panes, stats, *more,
):
    stages = cols_n.bit_length() - 1
    recvs, more = more[:stages], more[stages:]
    (own_sem, raw_sem, zsend, zrecv, csend, crecv, cfree, hsend, hrecv, hfree) = more[:10]
    (lower_sem, fzsend, fzrecv, fsend, frecv, tile_sem, msend, mrecv, pane_sem, ssem, rsem) = more[10:]
    _, _, _, wide, _ = factor_ref.shape
    span = tile.shape[1]
    outer = mirror_ref.shape[2]
    ratio = cols_n // rows_n
    cycles, _, groups, blk, lanes_n = land.shape
    depth = groups * lanes_n
    share = right.shape[0]
    half_rows = sums.shape[2]
    blocks, part = raw.shape[1], raw.shape[3]
    half = cols_n // 2
    orders = halvings(cols_n)
    z, c = lax.axis_index("row"), lax.axis_index("col")

    def peer(bit):
        return lax.bitwise_xor(c, jnp.int32(1 << bit))

    def cyc_of(it):
        return cycles - 1 - it

    barrier = pltpu.get_barrier_semaphore()
    me = z * cols_n + c
    everyone = rows_n * cols_n

    def greet(step, _):
        other = lax.rem(me + step, everyone)
        pl.semaphore_signal(
            barrier, inc=1, device_id=(other // cols_n, lax.rem(other, cols_n)), device_id_type=MESH
        )
        return 0

    lax.fori_loop(1, everyone, greet, 0)
    own = pltpu.make_async_copy(below_ref, land.at[:, z], own_sem)
    own.start()
    lower = pltpu.make_async_copy(lower_ref, factor_ref.at[:, z, c], lower_sem)
    lower.start()

    def m_of(k):
        return jnp.where(k < half, cols_n - 1 - 2 * k, 2 * (cols_n - 1 - k))

    def raw_copy(k, slot):
        s = lax.bitwise_xor(m_of(k), c)
        group = s * part // blk * blocks
        begin = pl.multiple_of(lax.rem(s * part, blk), part)
        return pltpu.make_async_copy(
            rest_ref.at[pl.ds(group, blocks), :, pl.ds(begin, part)], raw.at[slot], raw_sem.at[slot]
        )

    raw_copy(0, 0).start()
    own.wait()
    lower.wait()
    pl.semaphore_wait(barrier, everyone - 1)

    def piece(kind, cyc, source, to, way):
        block = factor_ref.at[cyc, source, c] if kind else land.at[cyc, source]
        return pltpu.make_async_remote_copy(
            src_ref=block,
            dst_ref=block,
            send_sem=(fzsend if kind else zsend).at[cyc, source, way],
            recv_sem=(fzrecv if kind else zrecv).at[cyc, source],
            device_id=(to, c),
            device_id_type=MESH,
        )

    def send_own(cyc):
        for kind in range(2):
            @pl.when(z < rows_n - 1)
            def _():
                piece(kind, cyc, z, z + 1, 0).start()

            @pl.when(z > 0)
            def _():
                piece(kind, cyc, z, z - 1, 1).start()

    inner = (z > 0) & (z < rows_n - 1)

    def arrive(cyc, forward):
        for t in range(1, rows_n):
            for kind in range(2):
                @pl.when((z >= t) & (inner == forward))
                def _():
                    piece(kind, cyc, z - t, z, 0).wait_recv()
                    if forward:
                        piece(kind, cyc, z - t, z + 1, 0).start()

                @pl.when((z + t < rows_n) & (inner == forward))
                def _():
                    piece(kind, cyc, z + t, z, 0).wait_recv()
                    if forward:
                        piece(kind, cyc, z + t, z - 1, 1).start()

    def relay(cyc):
        arrive(cyc, True)

        @pl.when(inner & (cyc > 0))
        def _():
            send_own(cyc - 1)

    @pl.when(inner)
    def _():
        send_own(cycles - 1)

    @pl.when(jnp.logical_not(inner))
    def _():
        for at in range(cycles):
            send_own(cycles - 1 - at)

    relay(cycles - 1)

    def pane_copy(at, slot):
        return pltpu.make_async_copy(matrix_ref.at[at], panes.at[slot], pane_sem.at[slot])

    pane_copy(0, 0).start()
    squares[...] = jnp.zeros_like(squares)

    def pane_step(at, _):
        slot = lax.rem(at, 2)
        pane_copy(at, slot).wait()

        @pl.when(at + 1 < matrix_ref.shape[0])
        def _():
            pane_copy(at + 1, 1 - slot).start()

        value = panes[slot].reshape(-1, 8, lanes_n)
        squares[0] += jnp.sum(value * value, axis=0)
        return 0

    lax.fori_loop(0, matrix_ref.shape[0], pane_step, 0)

    def spread(cyc, source, to, at):
        return pltpu.make_async_remote_copy(
            src_ref=factor_ref.at[cyc, :, source],
            dst_ref=factor_ref.at[cyc, :, source],
            send_sem=fsend.at[cyc, at],
            recv_sem=frecv.at[cyc, at],
            device_id=(z, to),
            device_id_type=MESH,
        )

    def factor_start(cyc):
        for e in [1] + list(range(2, cols_n, 2)):
            spread(cyc, c, lax.bitwise_xor(c, jnp.int32(e)), e).start()

    def factor_pass(cyc):
        for e in range(2, cols_n, 2):
            other = lax.bitwise_xor(c, jnp.int32(e))
            spread(cyc, other, other, e).wait_recv()
            spread(cyc, other, peer(0), e ^ 1).start()

    def factor_wait(cyc):
        for e in range(1, cols_n, 2):
            other = lax.bitwise_xor(c, jnp.int32(e))
            spread(cyc, other, other, e).wait_recv()

    def away(cyc, to, turn):
        return pltpu.make_async_remote_copy(
            src_ref=outbox.at[to, turn],
            dst_ref=mirror_ref.at[cyc, c],
            send_sem=msend.at[to, turn],
            recv_sem=mrecv.at[cyc, c],
            device_id=(to, turn * rows_n + z),
            device_id_type=MESH,
        )

    def at_home(cyc, to, turn):
        return pltpu.make_async_copy(
            outbox.at[to, turn], mirror_ref.at[cyc, c], msend.at[to, turn]
        )

    def is_home(to, turn):
        return (z == to) & (turn * rows_n + z == c)

    def mail_wait(cyc):
        for to in range(rows_n):
            for turn in range(ratio):
                @pl.when(is_home(to, turn))
                def _():
                    at_home(cyc, to, turn).wait()

                @pl.when(jnp.logical_not(is_home(to, turn)))
                def _():
                    away(cyc, to, turn).wait_send()

    def panel_step(it):
        cyc = cyc_of(it)
        factor_wait(cyc)

        def tile_step(back, _):
            from_cyc = cycles - 1 - back
            copy = pltpu.make_async_copy(
                factor_ref.at[from_cyc, :, pl.ds(cyc * span, span)], tile, tile_sem
            )
            copy.start()
            copy.wait()
            for source in range(rows_n):
                for column in range(span):
                    value = tile[source, column]
                    high = value.astype(jnp.bfloat16)
                    low = (value - high.astype(jnp.float32)).astype(jnp.bfloat16)
                    rows = slice(column * wide, (column + 1) * wide)
                    cols = slice(source * blk, (source + 1) * blk)
                    pair[0, rows, cols] = high
                    pair[1, rows, cols] = low
            product = None
            for one, two in ((0, 0), (0, 1), (1, 0)):
                term = jnp.dot(pair[one], update[from_cyc, two], preferred_element_type=jnp.float32)
                product = term if product is None else product + term

            @pl.when(back == 0)
            def _():
                total[...] = product

            @pl.when(back > 0)
            def _():
                total[...] += product

            return 0

        lax.fori_loop(0, it + 1, tile_step, 0)

        @pl.when(it > 0)
        def _():
            mail_wait(cyc + 1)

        for to in range(rows_n):
            value = total[to * blk : (to + 1) * blk, :]
            square = value * value
            partial = jnp.sum(square.reshape(blk // 8, 8, share), axis=0)
            for lane in range(0, share, lanes_n):
                squares[1] += partial[:, lane : lane + lanes_n]
            for turn in range(ratio):
                for place in range(outer):
                    begin = (place * ratio + turn) * part
                    outbox[to, turn, place] = value[:, begin : begin + part]
        for to in range(rows_n):
            for turn in range(ratio):
                @pl.when(is_home(to, turn))
                def _():
                    at_home(cyc, to, turn).start()

                @pl.when(jnp.logical_not(is_home(to, turn)))
                def _():
                    away(cyc, to, turn).start()

    def core_copy(m):
        slot = m // 2
        return pltpu.make_async_remote_copy(
            src_ref=sums.at[:, m],
            dst_ref=recvs[0].at[:, slot],
            send_sem=csend.at[slot],
            recv_sem=crecv.at[slot],
            device_id=(z, peer(0)),
            device_id_type=MESH,
        )

    where = {}
    for stage in range(1, stages):
        for stream in range(2):
            for slot, m in enumerate(held(orders[stream], stage, cols_n)):
                where[stage, stream, m] = (slot, len(where))

    def hop(stage, stream, m):
        bit = orders[stream][stage]
        slot, at = where[stage, stream, m]
        return pltpu.make_async_remote_copy(
            src_ref=sums.at[stream, m | (1 << bit)],
            dst_ref=recvs[stage].at[stream, slot],
            send_sem=hsend.at[at],
            recv_sem=hrecv.at[at],
            device_id=(z, peer(bit)),
            device_id_type=MESH,
        )

    def start_hop(stage, stream, m, it):
        at = where[stage, stream, m][1]

        @pl.when(it > 0)
        def _():
            pl.semaphore_wait(hfree.at[at], 1)

        hop(stage, stream, m).start()

    def sends_of(stage, stream):
        return [m for m in held(orders[stream], stage, cols_n)]

    def finish_hop(stage, stream, m, it, last):
        bit = orders[stream][stage]
        slot, at = where[stage, stream, m]
        hop(stage, stream, m).wait()
        added = sums[stream, m] + recvs[stage][stream, slot]
        if last:
            high = added.astype(jnp.bfloat16)
            rows = slice(stream * half_rows, (stream + 1) * half_rows)
            update[cyc_of(it), 0, rows] = high
            update[cyc_of(it), 1, rows] = (added - high.astype(jnp.float32)).astype(jnp.bfloat16)
        else:
            sums[stream, m] = added

        @pl.when(it < cycles - 1)
        def _():
            pl.semaphore_signal(hfree.at[at], inc=1, device_id=(z, peer(bit)), device_id_type=MESH)

        if not last:
            following = orders[stream][stage + 1]
            if m & (1 << following):
                start_hop(stage + 1, stream, m ^ (1 << following), it)

    def finish_last(it):
        for stream in range(2):
            finish_hop(stages - 1, stream, 0, it, True)
        panel_step(it)

    def chunk(it, _):
        cyc = cyc_of(it)
        arrive(cyc, False)
        factor_start(cyc)

        def split_left(source, _):
            rows = pl.ds(pl.multiple_of(source * blk, blk), blk)
            for group in range(groups):
                value = -land[cyc, source, group]
                high = value.astype(jnp.bfloat16)
                low = (value - high.astype(jnp.float32)).astype(jnp.bfloat16)
                cols = group * lanes_n
                left[rows, cols : cols + lanes_n] = high
                left[rows, depth + cols : depth + cols + lanes_n] = low
                left[rows, 2 * depth + cols : 2 * depth + cols + lanes_n] = high
            return 0

        lax.fori_loop(0, rows_n, split_left, 0)

        def share_step(k, _):
            m = m_of(k)
            s = lax.bitwise_xor(m, c)
            at = it * cols_n + k
            slot = lax.rem(at, 2)
            raw_copy(k, slot).wait()

            @pl.when(at + 1 < cycles * cols_n)
            def _():
                raw_copy(lax.rem(k + 1, cols_n), 1 - slot).start()

            for group in range(groups):
                value = raw[slot, :, group].reshape(share, lanes_n)
                high = value.astype(jnp.bfloat16)
                low = (value - high.astype(jnp.float32)).astype(jnp.bfloat16)
                cols = group * lanes_n
                right[:, cols : cols + lanes_n] = high
                right[:, depth + cols : depth + cols + lanes_n] = high
                right[:, 2 * depth + cols : 2 * depth + cols + lanes_n] = low

            @pl.when(it == 0)
            def _():
                for group in range(groups):
                    value = raw[slot, :, group].reshape(-1, 8, lanes_n)
                    squares[1] += jnp.sum(value * value, axis=0)

            @pl.when(k == half)
            def _():
                @pl.when(it > 0)
                def _():
                    finish_last(it - 1)

                @pl.when(it + 1 < cycles)
                def _():
                    relay(cyc - 1)

            @pl.when((k < half) & (it > 0))
            def _():
                core_copy(m).wait_send()

            product = lax.dot_general(
                left[...], right[...], (((1,), (1,)), ((), ())),
                preferred_element_type=jnp.float32,
            )
            sums[0, m] = product[:half_rows]
            sums[1, m] = product[half_rows:]

            turn = cyc - c // rows_n
            mine = (s < steps_of) & (lax.rem(turn + ratio * cycles, ratio) == 0)

            @pl.when(mine)
            def _():
                begin = lax.rem(c, rows_n) * blk
                stream = begin // half_rows
                rows = pl.ds(pl.multiple_of(lax.rem(begin, half_rows), blk), blk)
                mark = lax.rem(lax.rem(turn + ratio * cycles, ratio * cycles) // ratio, upper_ref.shape[0])
                sums[stream, m, rows, :] += upper_ref[mark, jnp.minimum(s, steps_of - 1)]

            @pl.when(k < half)
            def _():
                @pl.when(it > 0)
                def _():
                    pl.semaphore_wait(cfree.at[m // 2], 1)

                core_copy(m).start()

            @pl.when(k >= half)
            def _():
                core_copy(m + 1).wait_recv()
                for stream in range(2):
                    sums[stream, m] += recvs[0][stream, m // 2]

                @pl.when(it < cycles - 1)
                def _():
                    pl.semaphore_signal(
                        cfree.at[m // 2], inc=1, device_id=(z, peer(0)), device_id_type=MESH
                    )

                for stream in range(2):
                    bit = orders[stream][1]
                    for target in held(orders[stream], 1, cols_n):
                        @pl.when(m == target | (1 << bit))
                        def _():
                            start_hop(1, stream, target, it)

            return 0

        lax.fori_loop(0, cols_n, share_step, 0)
        for stage in range(1, stages - 1):
            for stream in range(2):
                order = sorted(
                    held(orders[stream], stage, cols_n),
                    key=lambda m: 0 if m & (1 << orders[stream][stage + 1]) else 1,
                )
                for m in order:
                    finish_hop(stage, stream, m, it, False)
        factor_pass(cyc)
        return 0

    lax.fori_loop(0, cycles, chunk, 0)
    finish_last(cycles - 1)
    stats[me] = squares[...]

    def report(other):
        return pltpu.make_async_remote_copy(
            src_ref=squares,
            dst_ref=stats.at[me],
            send_sem=ssem,
            recv_sem=rsem,
            device_id=(other // cols_n, lax.rem(other, cols_n)),
            device_id_type=MESH,
        )

    def tell(step, _):
        report(lax.rem(me + step, everyone)).start()
        return 0

    lax.fori_loop(1, everyone, tell, 0)
    for slot in range(half):
        core_copy(2 * slot + 1).wait_send()

    def drain(at, _):
        cyc = cyc_of(at)

        @pl.when(z < rows_n - 1)
        def _():
            for t in range(rows_n):
                @pl.when(z >= t)
                def _():
                    for kind in range(2):
                        piece(kind, cyc, z - t, z + 1, 0).wait_send()

        @pl.when(z > 0)
        def _():
            for t in range(rows_n):
                @pl.when(z + t < rows_n)
                def _():
                    for kind in range(2):
                        piece(kind, cyc, z + t, z - 1, 1).wait_send()

        for e in range(1, cols_n):
            spread(cyc, c, c, e).wait_send()
        for source in range(cols_n):
            @pl.when(jnp.logical_not((source == c) & (lax.rem(c, rows_n) == z)))
            def _():
                pltpu.make_async_remote_copy(
                    src_ref=mirror_ref.at[cyc, source],
                    dst_ref=mirror_ref.at[cyc, source],
                    send_sem=msend.at[0, 0],
                    recv_sem=mrecv.at[cyc, source],
                    device_id=(z, c),
                    device_id_type=MESH,
                ).wait_recv()

        return 0

    lax.fori_loop(0, cycles, drain, 0)
    mail_wait(0)
    every = stats.at[pl.ds(0, everyone - 1)]
    reports = pltpu.make_async_remote_copy(
        src_ref=every, dst_ref=every, send_sem=ssem, recv_sem=rsem,
        device_id=(z, c), device_id_type=MESH,
    )
    reports.wait_recv()
    reports.wait_send()
    total_ref[...] = jnp.sum(stats[...], axis=0)


def mirrored_panel(
    matrix, inverse_rest, lower_below, upper_block, lower_inverse, row_devices, col_devices
):
    row_cycles, blk, groups, lanes_n = inverse_rest.shape
    cycles = lower_below.shape[0]
    depth = groups * lanes_n
    share = row_cycles * blk // col_devices
    blocks = max(share // blk, col_devices // row_devices)
    part = share // blocks
    upper_cycles = upper_block.shape[2]
    stages = col_devices.bit_length() - 1
    steps_of = cycles * blk // share
    half_rows = row_devices * blk // 2
    upper = upper_block.reshape(cycles // blocks, blocks, blk // part, part, upper_cycles, blk)
    upper = upper.transpose(4, 0, 2, 5, 1, 3).reshape(upper_cycles, steps_of, blk, share)
    wide = lower_inverse.shape[2]
    ratio = col_devices // row_devices
    outer = blocks // ratio
    orders = halvings(col_devices)
    hops = sum(len(held(orders[0], stage, col_devices)) for stage in range(1, stages)) * 2
    rows = row_devices * blk
    scratch = [
        pltpu.VMEM((cycles, row_devices, groups, blk, lanes_n), jnp.float32),
        pltpu.VMEM((2, blocks, groups, part, lanes_n), jnp.float32),
        pltpu.VMEM((rows, 3 * depth), jnp.bfloat16),
        pltpu.VMEM((share, 3 * depth), jnp.bfloat16),
        pltpu.VMEM((2, col_devices, half_rows, share), jnp.float32),
        pltpu.VMEM((cycles, 2, rows, share), jnp.bfloat16),
        pltpu.VMEM((2, rows, rows), jnp.bfloat16),
        pltpu.VMEM((row_devices, rows // wide, wide, blk), jnp.float32),
        pltpu.VMEM((rows, share), jnp.float32),
        pltpu.VMEM((row_devices, ratio, outer, blk, part), jnp.float32),
        pltpu.VMEM((2, 8, lanes_n), jnp.float32),
        pltpu.VMEM((2,) + matrix.shape[1:], jnp.float32),
        pltpu.VMEM((row_devices * col_devices, 2, 8, lanes_n), jnp.float32),
    ]
    for stage in range(stages):
        scratch.append(pltpu.VMEM((2, col_devices >> (stage + 1), half_rows, share), jnp.float32))
    scratch += [
        pltpu.SemaphoreType.DMA,
        pltpu.SemaphoreType.DMA((2,)),
        pltpu.SemaphoreType.DMA((cycles, row_devices, 2)),
        pltpu.SemaphoreType.DMA((cycles, row_devices)),
        pltpu.SemaphoreType.DMA((col_devices // 2,)),
        pltpu.SemaphoreType.DMA((col_devices // 2,)),
        pltpu.SemaphoreType.REGULAR((col_devices // 2,)),
        pltpu.SemaphoreType.DMA((hops,)),
        pltpu.SemaphoreType.DMA((hops,)),
        pltpu.SemaphoreType.REGULAR((hops,)),
        pltpu.SemaphoreType.DMA,
        pltpu.SemaphoreType.DMA((cycles, row_devices, 2)),
        pltpu.SemaphoreType.DMA((cycles, row_devices)),
        pltpu.SemaphoreType.DMA((cycles, col_devices)),
        pltpu.SemaphoreType.DMA((cycles, col_devices)),
        pltpu.SemaphoreType.DMA,
        pltpu.SemaphoreType.DMA((row_devices, ratio)),
        pltpu.SemaphoreType.DMA((cycles, col_devices)),
        pltpu.SemaphoreType.DMA((2,)),
        pltpu.SemaphoreType.DMA,
        pltpu.SemaphoreType.DMA,
    ]
    mirror, _, totals = pl.pallas_call(
        functools.partial(panel_kernel, row_devices, col_devices, steps_of),
        out_shape=(
            jax.ShapeDtypeStruct((cycles, col_devices, outer, blk, part), jnp.float32),
            jax.ShapeDtypeStruct((cycles, row_devices, col_devices, wide, blk), jnp.float32),
            jax.ShapeDtypeStruct((2, 8, lanes_n), jnp.float32),
        ),
        in_specs=[
            pl.BlockSpec(memory_space=pltpu.HBM),
            pl.BlockSpec(memory_space=pltpu.HBM),
            pl.BlockSpec(memory_space=pltpu.HBM),
            pl.BlockSpec(memory_space=pltpu.VMEM),
            pl.BlockSpec(memory_space=pltpu.VMEM),
        ],
        out_specs=(
            pl.BlockSpec(memory_space=pltpu.HBM),
            pl.BlockSpec(memory_space=pltpu.HBM),
            pl.BlockSpec(memory_space=pltpu.VMEM),
        ),
        scratch_shapes=scratch,
        compiler_params=pltpu.CompilerParams(
            collective_id=0, has_side_effects=True, vmem_limit_bytes=66_000_000
        ),
        cost_estimate=pl.CostEstimate(
            flops=6 * cycles * rows * share * col_devices * depth,
            bytes_accessed=4 * cycles * col_devices * share * depth,
            transcendentals=0,
        ),
    )(
        matrix,
        inverse_rest.transpose(0, 2, 1, 3),
        lower_below.transpose(0, 2, 1, 3),
        upper,
        lower_inverse.transpose(0, 2, 1),
    )
    return mirror, totals


def per_device(matrix, inverse_rest, upper_block, lower_below, lower_inverse):
    row_devices = lax.axis_size("row")
    col_devices = lax.axis_size("col")
    row_cycles, blk_size, col_cycles, _ = matrix.shape
    panel_cycles = lower_inverse.shape[0]
    mirror, totals = mirrored_panel(
        matrix, inverse_rest, lower_below, upper_block, lower_inverse, row_devices, col_devices
    )
    inverse_block = mirror.transpose(0, 3, 1, 2, 4).reshape(
        panel_cycles, blk_size, col_cycles, blk_size
    )
    matrix_total, inverse_total = jnp.sum(totals[0]), jnp.sum(totals[1])
    balance = jnp.sqrt(jnp.sqrt(inverse_total / matrix_total))
    return 0.5 * (balance * matrix[:panel_cycles] + inverse_block / balance)


def solution(mesh):
    in_specs = (
        P(None, "row", None, "col"),
        P(None, "row", None, "col"),
        P(None, "row", None, "col"),
        P(None, "row", None, "col"),
        P(None, "row", "col"),
    )
    out_specs = P(None, "row", None, "col")
    return jax.shard_map(
        per_device, mesh=mesh, in_specs=in_specs, out_specs=out_specs, check_vma=False
    )
```

```python
import functools

import jax
import jax.numpy as jnp
from jax import lax
from jax.experimental import pallas as pl
from jax.experimental.pallas import tpu as pltpu
from jax.sharding import PartitionSpec as P

MESH = pl.DeviceIdType.MESH
CUTS = 2
AHEAD = 1
PANES = 4


def halvings(col_devices):
    bits = col_devices.bit_length() - 1
    return [[0] + list(range(1, bits)), [0] + list(range(bits - 1, 0, -1))]


def held(order, stage, col_devices):
    cleared = sum(1 << b for b in order[: stage + 1])
    return [m for m in range(col_devices) if m & cleared == 0]


def panel_kernel(
    rows_n, cols_n, steps_of,
    matrix_ref, rest_ref, below_ref, upper_ref, lower_ref, mirror_ref, factor_ref, total_ref,
    land, raw, left, right, sums, update, pair, tile, total, outbox, squares, panes, stats, *more,
):
    stages = cols_n.bit_length() - 1
    recvs, more = more[:stages], more[stages:]
    (own_sem, raw_sem, zsend, zrecv, csend, crecv, cfree, hsend, hrecv, hfree) = more[:10]
    (lower_sem, fzsend, fzrecv, fsend, frecv, tile_sem, msend, mrecv, pane_sem, ssem, rsem) = more[10:]
    _, _, _, wide, _ = factor_ref.shape
    span = tile.shape[1]
    outer = mirror_ref.shape[2]
    ratio = cols_n // rows_n
    units, _, groups, slim, lanes_n = land.shape
    cycles, blk = mirror_ref.shape[0], mirror_ref.shape[3]
    cuts = units // cycles
    depth = groups * lanes_n
    share = right.shape[0]
    half_rows = sums.shape[2]
    blocks, part = raw.shape[1], raw.shape[3]
    half = cols_n // 2
    ahead = min(AHEAD, units)
    orders = halvings(cols_n)
    z, c = lax.axis_index("row"), lax.axis_index("col")

    def peer(bit):
        return lax.bitwise_xor(c, jnp.int32(1 << bit))

    def cyc_of(it):
        return cycles - 1 - it // cuts

    barrier = pltpu.get_barrier_semaphore()
    me = z * cols_n + c
    everyone = rows_n * cols_n

    def greet(step, _):
        other = lax.rem(me + step, everyone)
        pl.semaphore_signal(
            barrier, inc=1, device_id=(other // cols_n, lax.rem(other, cols_n)), device_id_type=MESH
        )
        return 0

    lax.fori_loop(1, everyone, greet, 0)
    own = []
    for at in range(units):
        own.append(pltpu.make_async_copy(
            below_ref.at[cycles - 1 - at // cuts, :, pl.ds(at % cuts * slim, slim)],
            land.at[at, z], own_sem.at[at],
        ))
        own[at].start()
    lower = pltpu.make_async_copy(lower_ref, factor_ref.at[:, z, c], lower_sem)
    lower.start()

    def m_of(k):
        return jnp.where(k < half, cols_n - 1 - 2 * k, 2 * (cols_n - 1 - k))

    def raw_copy(k, slot):
        s = lax.bitwise_xor(m_of(k), c)
        group = s * part // blk * blocks
        begin = pl.multiple_of(lax.rem(s * part, blk), part)
        return pltpu.make_async_copy(
            rest_ref.at[pl.ds(group, blocks), :, pl.ds(begin, part)], raw.at[slot], raw_sem.at[slot]
        )

    raw_copy(0, 0).start()
    for at in range(units):
        own[at].wait()
    lower.wait()
    pl.semaphore_wait(barrier, everyone - 1)

    def piece(at, source, to, way):
        return pltpu.make_async_remote_copy(
            src_ref=land.at[at, source],
            dst_ref=land.at[at, source],
            send_sem=zsend.at[at, source, way],
            recv_sem=zrecv.at[at, source],
            device_id=(to, c),
            device_id_type=MESH,
        )

    def factor_piece(_, source, to, way):
        return pltpu.make_async_remote_copy(
            src_ref=factor_ref.at[:, source, c],
            dst_ref=factor_ref.at[:, source, c],
            send_sem=fzsend.at[source, way],
            recv_sem=fzrecv.at[source],
            device_id=(to, c),
            device_id_type=MESH,
        )

    def send_own(at, piece=piece):
        @pl.when(z < rows_n - 1)
        def _():
            piece(at, z, z + 1, 0).start()

        @pl.when(z > 0)
        def _():
            piece(at, z, z - 1, 1).start()

    inner = (z > 0) & (z < rows_n - 1)

    def arrive(at, forward, piece=piece):
        for t in range(1, rows_n):
            @pl.when((z >= t) & (inner == forward))
            def _():
                piece(at, z - t, z, 0).wait_recv()
                if forward:
                    piece(at, z - t, z + 1, 0).start()

            @pl.when((z + t < rows_n) & (inner == forward))
            def _():
                piece(at, z + t, z, 0).wait_recv()
                if forward:
                    piece(at, z + t, z - 1, 1).start()

    def lead(t):
        return ahead + rows_n - 2 - t

    def relay(at, t):
        @pl.when(inner & (z >= t))
        def _():
            piece(at, z - t, z, 0).wait_recv()
            piece(at, z - t, z + 1, 0).start()

        @pl.when(inner & (z + t < rows_n))
        def _():
            piece(at, z + t, z, 0).wait_recv()
            piece(at, z + t, z - 1, 1).start()

        if t == 1:
            @pl.when(inner & (at + 1 < units))
            def _():
                send_own(at + 1)

    def relay_first(begin, end):
        for at in range(begin, min(end, units)):
            for t in range(1, rows_n - 1):
                if at < lead(t):
                    relay(at, t)

    def relay_later(it):
        for t in range(rows_n - 2, 0, -1):
            @pl.when(it + lead(t) < units)
            def _():
                relay(it + lead(t), t)

    def spread(cyc, source, to, at):
        return pltpu.make_async_remote_copy(
            src_ref=factor_ref.at[cyc, :, source],
            dst_ref=factor_ref.at[cyc, :, source],
            send_sem=fsend.at[cyc, at],
            recv_sem=frecv.at[cyc, at],
            device_id=(z, to),
            device_id_type=MESH,
        )

    def used(cyc, source):
        return source * wide < (cyc + 1) * (rows_n * blk)

    def factor_start(cyc):
        for e in [1] + list(range(2, cols_n, 2)):
            @pl.when(used(cyc, c))
            def _():
                spread(cyc, c, lax.bitwise_xor(c, jnp.int32(e)), e).start()

    def factor_pass(cyc):
        for e in range(2, cols_n, 2):
            other = lax.bitwise_xor(c, jnp.int32(e))

            @pl.when(used(cyc, other))
            def _():
                spread(cyc, other, other, e).wait_recv()
                spread(cyc, other, peer(0), e ^ 1).start()

    def factor_wait(cyc):
        for e in range(1, cols_n, 2):
            other = lax.bitwise_xor(c, jnp.int32(e))

            @pl.when(used(cyc, other))
            def _():
                spread(cyc, other, other, e).wait_recv()

    def factor_sent(cyc):
        for e in [1] + list(range(2, cols_n, 2)):
            @pl.when(used(cyc, c))
            def _():
                spread(cyc, c, c, e).wait_send()

        for e in range(2, cols_n, 2):
            @pl.when(used(cyc, lax.bitwise_xor(c, jnp.int32(e))))
            def _():
                spread(cyc, c, c, e ^ 1).wait_send()

    early = range(cycles - 1, max(cycles - 3, -1), -1)

    send_own(0, factor_piece)

    @pl.when(inner)
    def _():
        send_own(0)

    @pl.when(jnp.logical_not(inner))
    def _():
        for at in range(units):
            send_own(at)

    arrive(0, True, factor_piece)

    @pl.when(inner)
    def _():
        for at in early:
            factor_start(at)

    relay_first(0, 1)

    def pane_copy(at, slot):
        return pltpu.make_async_copy(matrix_ref.at[at], panes.at[slot], pane_sem.at[slot])

    depth_of = panes.shape[0]
    for at in range(depth_of - 1):
        pane_copy(at, at).start()
    squares[...] = jnp.zeros_like(squares)

    def pane_step(at, _):
        slot = lax.rem(at, depth_of)
        later = at + depth_of - 1
        pane_copy(at, slot).wait()

        @pl.when(later < matrix_ref.shape[0])
        def _():
            pane_copy(later, lax.rem(later, depth_of)).start()

        value = panes[slot].reshape(-1, 8, lanes_n)
        squares[0] += jnp.sum(value * value, axis=0)
        return 0

    lax.fori_loop(0, matrix_ref.shape[0], pane_step, 0)

    arrive(0, False, factor_piece)

    @pl.when(jnp.logical_not(inner))
    def _():
        for at in early:
            factor_start(at)

    relay_first(1, lead(1))

    def away(cyc, to, turn):
        return pltpu.make_async_remote_copy(
            src_ref=outbox.at[cyc, to, turn],
            dst_ref=mirror_ref.at[cyc, c],
            send_sem=msend.at[cyc, to, turn],
            recv_sem=mrecv.at[cyc, c],
            device_id=(to, turn * rows_n + z),
            device_id_type=MESH,
        )

    def at_home(cyc, to, turn):
        return pltpu.make_async_copy(
            outbox.at[cyc, to, turn], mirror_ref.at[cyc, c], msend.at[cyc, to, turn]
        )

    def is_home(to, turn):
        return (z == to) & (turn * rows_n + z == c)

    def mail_wait(cyc):
        for to in range(rows_n):
            for turn in range(ratio):
                @pl.when(is_home(to, turn))
                def _():
                    at_home(cyc, to, turn).wait()

                @pl.when(jnp.logical_not(is_home(to, turn)))
                def _():
                    away(cyc, to, turn).wait_send()

    def tiles(cyc, first, last):
        def tile_step(back, _):
            from_cyc = cycles - 1 - back
            copy = pltpu.make_async_copy(
                factor_ref.at[from_cyc, :, pl.ds(cyc * span, span)], tile, tile_sem
            )
            copy.start()
            copy.wait()
            for source in range(rows_n):
                for column in range(span):
                    value = tile[source, column]
                    high = value.astype(jnp.bfloat16)
                    low = (value - high.astype(jnp.float32)).astype(jnp.bfloat16)
                    rows = slice(column * wide, (column + 1) * wide)
                    cols = slice(source * blk, (source + 1) * blk)
                    pair[0, rows, cols] = high
                    pair[1, rows, cols] = low
            product = None
            for one, two in ((0, 0), (0, 1), (1, 0)):
                term = jnp.dot(pair[one], update[from_cyc, two], preferred_element_type=jnp.float32)
                product = term if product is None else product + term

            @pl.when(back == 0)
            def _():
                total[...] = product

            @pl.when(back > 0)
            def _():
                total[...] += product

            return 0

        lax.fori_loop(first, last, tile_step, 0)

    def fill(cyc):

        for to in range(rows_n):
            value = total[to * blk : (to + 1) * blk, :]
            square = value * value
            partial = jnp.sum(square.reshape(blk // 8, 8, share), axis=0)
            for lane in range(0, share, lanes_n):
                squares[1] += partial[:, lane : lane + lanes_n]
            for turn in range(ratio):
                for place in range(outer):
                    begin = (place * ratio + turn) * part
                    outbox[cyc, to, turn, place] = value[:, begin : begin + part]

    def mail(cyc):
        for to in range(rows_n):
            for turn in range(ratio):
                @pl.when(is_home(to, turn))
                def _():
                    at_home(cyc, to, turn).start()

                @pl.when(jnp.logical_not(is_home(to, turn)))
                def _():
                    away(cyc, to, turn).start()

    def core_copy(m):
        slot = m // 2
        return pltpu.make_async_remote_copy(
            src_ref=sums.at[:, m],
            dst_ref=recvs[0].at[:, slot],
            send_sem=csend.at[slot],
            recv_sem=crecv.at[slot],
            device_id=(z, peer(0)),
            device_id_type=MESH,
        )

    where = {}
    for stage in range(1, stages):
        for stream in range(2):
            for slot, m in enumerate(held(orders[stream], stage, cols_n)):
                where[stage, stream, m] = (slot, len(where))

    def hop(stage, stream, m):
        bit = orders[stream][stage]
        slot, at = where[stage, stream, m]
        return pltpu.make_async_remote_copy(
            src_ref=sums.at[stream, m | (1 << bit)],
            dst_ref=recvs[stage].at[stream, slot],
            send_sem=hsend.at[at],
            recv_sem=hrecv.at[at],
            device_id=(z, peer(bit)),
            device_id_type=MESH,
        )

    def start_hop(stage, stream, m, it):
        at = where[stage, stream, m][1]

        @pl.when(it > 0)
        def _():
            pl.semaphore_wait(hfree.at[at], 1)

        hop(stage, stream, m).start()

    def sends_of(stage, stream):
        return [m for m in held(orders[stream], stage, cols_n)]

    def finish_hop(stage, stream, m, it, last):
        bit = orders[stream][stage]
        slot, at = where[stage, stream, m]
        hop(stage, stream, m).wait()
        added = sums[stream, m] + recvs[stage][stream, slot]
        if last:
            high = added.astype(jnp.bfloat16)
            low = (added - high.astype(jnp.float32)).astype(jnp.bfloat16)
            for place in range(half_rows // slim):
                source = stream * (half_rows // slim) + place
                begin = pl.multiple_of(source * blk + lax.rem(it, cuts) * slim, slim)
                part_rows = slice(place * slim, (place + 1) * slim)
                update[cyc_of(it), 0, pl.ds(begin, slim)] = high[part_rows]
                update[cyc_of(it), 1, pl.ds(begin, slim)] = low[part_rows]
        else:
            sums[stream, m] = added

        @pl.when(it < units - 1)
        def _():
            pl.semaphore_signal(hfree.at[at], inc=1, device_id=(z, peer(bit)), device_id_type=MESH)

        if not last:
            following = orders[stream][stage + 1]
            if m & (1 << following):
                start_hop(stage + 1, stream, m ^ (1 << following), it)

    def finish_last(it):
        for stream in range(2):
            finish_hop(stages - 1, stream, 0, it, True)

        @pl.when(lax.rem(it, cuts) == cuts - 1)
        def _():
            factor_wait(cyc_of(it))
            tiles(cyc_of(it), 0, cycles - cyc_of(it))
            fill(cyc_of(it))

    def finish_mid(it):
        for stage in range(1, stages - 1):
            for stream in range(2):
                order = sorted(
                    held(orders[stream], stage, cols_n),
                    key=lambda m: 0 if m & (1 << orders[stream][stage + 1]) else 1,
                )
                for m in order:
                    finish_hop(stage, stream, m, it, False)

    def chunk(it, _):
        cyc = cyc_of(it)
        arrive(it, False)

        @pl.when(it == units - 1)
        def _():
            for at in range(cycles - 1, 0, -1):
                mail(at)

        @pl.when((it >= cuts) & (lax.rem(it, cuts) == 0) & (cyc > 0))
        def _():
            factor_start(cyc - 1)

        def split_left(source, _):
            rows = pl.ds(pl.multiple_of(source * slim, slim), slim)
            for group in range(groups):
                value = -land[it, source, group]
                high = value.astype(jnp.bfloat16)
                low = (value - high.astype(jnp.float32)).astype(jnp.bfloat16)
                cols = group * lanes_n
                left[rows, cols : cols + lanes_n] = high
                left[rows, depth + cols : depth + cols + lanes_n] = low
                left[rows, 2 * depth + cols : 2 * depth + cols + lanes_n] = high
            return 0

        lax.fori_loop(0, rows_n, split_left, 0)

        def share_step(k, _):
            m = m_of(k)
            s = lax.bitwise_xor(m, c)
            at = it * cols_n + k
            slot = lax.rem(at, 2)
            raw_copy(k, slot).wait()

            @pl.when(at + 1 < units * cols_n)
            def _():
                raw_copy(lax.rem(k + 1, cols_n), 1 - slot).start()

            for group in range(groups):
                value = raw[slot, :, group].reshape(share, lanes_n)
                high = value.astype(jnp.bfloat16)
                low = (value - high.astype(jnp.float32)).astype(jnp.bfloat16)
                cols = group * lanes_n
                right[:, cols : cols + lanes_n] = high
                right[:, depth + cols : depth + cols + lanes_n] = high
                right[:, 2 * depth + cols : 2 * depth + cols + lanes_n] = low

            @pl.when(it == 0)
            def _():
                for group in range(groups):
                    value = raw[slot, :, group].reshape(-1, 8, lanes_n)
                    squares[1] += jnp.sum(value * value, axis=0)

            @pl.when(k == half)
            def _():
                @pl.when(it > 0)
                def _():
                    finish_last(it - 1)

                relay_later(it)

            @pl.when((k == 1) & (it > 0))
            def _():
                finish_mid(it - 1)

            @pl.when((k < half) & (it > 0))
            def _():
                core_copy(m).wait_send()

            product = lax.dot_general(
                left[...], right[...], (((1,), (1,)), ((), ())),
                preferred_element_type=jnp.float32,
            )
            sums[0, m] = product[:half_rows]
            sums[1, m] = product[half_rows:]

            turn = cyc - c // rows_n
            mine = (s < steps_of) & (lax.rem(turn + ratio * cycles, ratio) == 0)

            @pl.when(mine)
            def _():
                begin = lax.rem(c, rows_n) * slim
                stream = begin // half_rows
                rows = pl.ds(pl.multiple_of(lax.rem(begin, half_rows), slim), slim)
                taken = pl.ds(pl.multiple_of(lax.rem(it, cuts) * slim, slim), slim)
                mark = lax.rem(lax.rem(turn + ratio * cycles, ratio * cycles) // ratio, upper_ref.shape[0])
                sums[stream, m, rows, :] += upper_ref[mark, jnp.minimum(s, steps_of - 1), taken]

            @pl.when(k < half)
            def _():
                @pl.when(it > 0)
                def _():
                    pl.semaphore_wait(cfree.at[m // 2], 1)

                core_copy(m).start()

            @pl.when(k >= half)
            def _():
                core_copy(m + 1).wait_recv()
                for stream in range(2):
                    sums[stream, m] += recvs[0][stream, m // 2]

                @pl.when(it < units - 1)
                def _():
                    pl.semaphore_signal(
                        cfree.at[m // 2], inc=1, device_id=(z, peer(0)), device_id_type=MESH
                    )

                for stream in range(2):
                    bit = orders[stream][1]
                    for target in held(orders[stream], 1, cols_n):
                        @pl.when(m == target | (1 << bit))
                        def _():
                            start_hop(1, stream, target, it)

            return 0

        lax.fori_loop(0, cols_n, share_step, 0)

        @pl.when(it == cuts - 1)
        def _():
            for at in early:
                factor_pass(at)

        @pl.when((it >= cuts) & (lax.rem(it, cuts) == cuts - 1) & (cyc > 0))
        def _():
            factor_pass(cyc - 1)

        return 0

    lax.fori_loop(0, units, chunk, 0)
    finish_mid(units - 1)
    factor_wait(0)
    tiles(0, 0, cycles - 1)
    for stream in range(2):
        finish_hop(stages - 1, stream, 0, units - 1, True)
    tiles(0, cycles - 1, cycles)
    fill(0)
    stats[me] = squares[...]

    def report(other):
        return pltpu.make_async_remote_copy(
            src_ref=squares,
            dst_ref=stats.at[me],
            send_sem=ssem,
            recv_sem=rsem,
            device_id=(other // cols_n, lax.rem(other, cols_n)),
            device_id_type=MESH,
        )

    def tell(step, _):
        report(lax.rem(me + step, everyone)).start()
        return 0

    lax.fori_loop(1, everyone, tell, 0)
    mail(0)
    for slot in range(half):
        core_copy(2 * slot + 1).wait_send()

    def sent(at, piece=piece):
        @pl.when(z < rows_n - 1)
        def _():
            for t in range(rows_n):
                @pl.when(z >= t)
                def _():
                    piece(at, z - t, z + 1, 0).wait_send()

        @pl.when(z > 0)
        def _():
            for t in range(rows_n):
                @pl.when(z + t < rows_n)
                def _():
                    piece(at, z + t, z - 1, 1).wait_send()

    def drain(at, _):
        sent(at)
        return 0

    lax.fori_loop(0, units, drain, 0)
    sent(0, factor_piece)
    def receive(cyc, _):
        mail_wait(cyc)
        factor_sent(cyc)
        for source in range(cols_n):
            @pl.when(jnp.logical_not((source == c) & (lax.rem(c, rows_n) == z)))
            def _():
                pltpu.make_async_remote_copy(
                    src_ref=mirror_ref.at[cyc, source],
                    dst_ref=mirror_ref.at[cyc, source],
                    send_sem=msend.at[0, 0, 0],
                    recv_sem=mrecv.at[cyc, source],
                    device_id=(z, c),
                    device_id_type=MESH,
                ).wait_recv()

        return 0

    lax.fori_loop(0, cycles, receive, 0)
    every = stats.at[pl.ds(0, everyone - 1)]
    reports = pltpu.make_async_remote_copy(
        src_ref=every, dst_ref=every, send_sem=ssem, recv_sem=rsem,
        device_id=(z, c), device_id_type=MESH,
    )
    reports.wait_recv()
    reports.wait_send()
    total_ref[...] = jnp.sum(stats[...], axis=0)


def mirrored_panel(
    matrix, inverse_rest, lower_below, upper_block, lower_inverse, row_devices, col_devices
):
    row_cycles, blk, groups, lanes_n = inverse_rest.shape
    cycles = lower_below.shape[0]
    depth = groups * lanes_n
    share = row_cycles * blk // col_devices
    blocks = max(share // blk, col_devices // row_devices)
    part = share // blocks
    upper_cycles = upper_block.shape[2]
    stages = col_devices.bit_length() - 1
    steps_of = cycles * blk // share
    cuts = CUTS
    half_rows = row_devices * blk // cuts // 2
    upper = upper_block.reshape(cycles // blocks, blocks, blk // part, part, upper_cycles, blk)
    upper = upper.transpose(4, 0, 2, 5, 1, 3).reshape(upper_cycles, steps_of, blk, share)
    wide = lower_inverse.shape[2]
    ratio = col_devices // row_devices
    outer = blocks // ratio
    orders = halvings(col_devices)
    hops = sum(len(held(orders[0], stage, col_devices)) for stage in range(1, stages)) * 2
    rows = row_devices * blk
    scratch = [
        pltpu.VMEM((cycles * cuts, row_devices, groups, blk // cuts, lanes_n), jnp.float32),
        pltpu.VMEM((2, blocks, groups, part, lanes_n), jnp.float32),
        pltpu.VMEM((rows // cuts, 3 * depth), jnp.bfloat16),
        pltpu.VMEM((share, 3 * depth), jnp.bfloat16),
        pltpu.VMEM((2, col_devices, half_rows, share), jnp.float32),
        pltpu.VMEM((cycles, 2, rows, share), jnp.bfloat16),
        pltpu.VMEM((2, rows, rows), jnp.bfloat16),
        pltpu.VMEM((row_devices, rows // wide, wide, blk), jnp.float32),
        pltpu.VMEM((rows, share), jnp.float32),
        pltpu.VMEM((cycles, row_devices, ratio, outer, blk, part), jnp.float32),
        pltpu.VMEM((2, 8, lanes_n), jnp.float32),
        pltpu.VMEM((PANES,) + matrix.shape[1:], jnp.float32),
        pltpu.VMEM((row_devices * col_devices, 2, 8, lanes_n), jnp.float32),
    ]
    for stage in range(stages):
        scratch.append(pltpu.VMEM((2, col_devices >> (stage + 1), half_rows, share), jnp.float32))
    scratch += [
        pltpu.SemaphoreType.DMA((cycles * cuts,)),
        pltpu.SemaphoreType.DMA((2,)),
        pltpu.SemaphoreType.DMA((cycles * cuts, row_devices, 2)),
        pltpu.SemaphoreType.DMA((cycles * cuts, row_devices)),
        pltpu.SemaphoreType.DMA((col_devices // 2,)),
        pltpu.SemaphoreType.DMA((col_devices // 2,)),
        pltpu.SemaphoreType.REGULAR((col_devices // 2,)),
        pltpu.SemaphoreType.DMA((hops,)),
        pltpu.SemaphoreType.DMA((hops,)),
        pltpu.SemaphoreType.REGULAR((hops,)),
        pltpu.SemaphoreType.DMA,
        pltpu.SemaphoreType.DMA((row_devices, 2)),
        pltpu.SemaphoreType.DMA((row_devices,)),
        pltpu.SemaphoreType.DMA((cycles, col_devices)),
        pltpu.SemaphoreType.DMA((cycles, col_devices)),
        pltpu.SemaphoreType.DMA,
        pltpu.SemaphoreType.DMA((cycles, row_devices, ratio)),
        pltpu.SemaphoreType.DMA((cycles, col_devices)),
        pltpu.SemaphoreType.DMA((PANES,)),
        pltpu.SemaphoreType.DMA,
        pltpu.SemaphoreType.DMA,
    ]
    mirror, _, totals = pl.pallas_call(
        functools.partial(panel_kernel, row_devices, col_devices, steps_of),
        out_shape=(
            jax.ShapeDtypeStruct((cycles, col_devices, outer, blk, part), jnp.float32),
            jax.ShapeDtypeStruct((cycles, row_devices, col_devices, wide, blk), jnp.float32),
            jax.ShapeDtypeStruct((2, 8, lanes_n), jnp.float32),
        ),
        in_specs=[
            pl.BlockSpec(memory_space=pltpu.HBM),
            pl.BlockSpec(memory_space=pltpu.HBM),
            pl.BlockSpec(memory_space=pltpu.HBM),
            pl.BlockSpec(memory_space=pltpu.VMEM),
            pl.BlockSpec(memory_space=pltpu.VMEM),
        ],
        out_specs=(
            pl.BlockSpec(memory_space=pltpu.HBM),
            pl.BlockSpec(memory_space=pltpu.HBM),
            pl.BlockSpec(memory_space=pltpu.VMEM),
        ),
        scratch_shapes=scratch,
        compiler_params=pltpu.CompilerParams(
            collective_id=0, has_side_effects=True, vmem_limit_bytes=66_000_000
        ),
        cost_estimate=pl.CostEstimate(
            flops=6 * cycles * rows * share * col_devices * depth,
            bytes_accessed=4 * cycles * col_devices * share * depth,
            transcendentals=0,
        ),
    )(
        matrix,
        inverse_rest.transpose(0, 2, 1, 3),
        lower_below.transpose(0, 2, 1, 3),
        upper,
        lower_inverse.transpose(0, 2, 1),
    )
    return mirror, totals


def per_device(matrix, inverse_rest, upper_block, lower_below, lower_inverse):
    row_devices = lax.axis_size("row")
    col_devices = lax.axis_size("col")
    row_cycles, blk_size, col_cycles, _ = matrix.shape
    panel_cycles = lower_inverse.shape[0]
    mirror, totals = mirrored_panel(
        matrix, inverse_rest, lower_below, upper_block, lower_inverse, row_devices, col_devices
    )
    inverse_block = mirror.transpose(0, 3, 1, 2, 4).reshape(
        panel_cycles, blk_size, col_cycles, blk_size
    )
    matrix_total, inverse_total = jnp.sum(totals[0]), jnp.sum(totals[1])
    balance = jnp.sqrt(jnp.sqrt(inverse_total / matrix_total))
    return 0.5 * (balance * matrix[:panel_cycles] + inverse_block / balance)


def solution(mesh):
    in_specs = (
        P(None, "row", None, "col"),
        P(None, "row", None, "col"),
        P(None, "row", None, "col"),
        P(None, "row", None, "col"),
        P(None, "row", "col"),
    )
    out_specs = P(None, "row", None, "col")
    return jax.shard_map(
        per_device, mesh=mesh, in_specs=in_specs, out_specs=out_specs, check_vma=False
    )
```
